512 devices in a mesh: cfg: 2 (over x_lo), ctx: 32 (over y, x_hi, core), tp: 8 (over z).
Axes of the slice: x: 4 (x_hi: 2, x_lo: 2; x = x_hi * 2 + x_lo), y: 8, z: 8, core: 2. Of those that a mesh axis runs over, the one named last changes fastest.
Arguments:
- query_proj: bfloat16 [2, 8192, 3072], P('cfg', 'ctx', 'tp'), may hold values from -8 to 8
- key_proj: bfloat16 [2, 8192, 3072], P('cfg', 'ctx', 'tp'), may hold values from -8 to 8
- value_proj: bfloat16 [2, 8192, 3072], P('cfg', 'ctx', 'tp'), may hold values from -6 to 6
- query_gain: float32 [128], replicated, may hold values from 1 to 8
- key_gain: float32 [128], replicated, may hold values from 1 to 8
- block_input: bfloat16 [2, 8192, 3072], P('cfg', ('ctx', 'tp')), may hold values from -120 to 120
- cached_out: bfloat16 [2, 8192, 3072], P('cfg', ('ctx', 'tp')), may hold values from -120 to 120
- replay_mask: int32 [2, 8192], P('cfg', 'ctx'), may hold values from 0 to 1, as said below
- branch_gate: float32 [2, 3072], P('cfg'), may hold values from 1 to 4
- attn_weight: bfloat16 [3072, 3072], P('tp'), may hold values from -0.109375 to 0.109375
- final_shift: float32 [2, 3072], P('cfg'), may hold values from -4 to 4
- final_scale: float32 [2, 3072], P('cfg'), may hold values from -2 to 2
- patch_weight: bfloat16 [3072, 64], replicated, may hold values from -0.109375 to 0.109375
Outputs:
- block_out: bfloat16 [2, 8192, 3072], P('cfg', ('ctx', 'tp'))
- velocity: float32 [8192, 64], P(('ctx', 'tp'), 'cfg')
The draws below stay inside these ranges and needn't reach their ends.
Inputs may be any that keep to these rules, and one draw needn't show every extreme that they name: `replay_mask`: in each branch, at most 128 of the 256 rows of one index of ctx have a 0, and some index of ctx has exactly 128.
All inputs are finite; a program needn't handle non-finite values.
Results may differ from the reference program's by a relative error of at most 0.0097.
Values may be sent and summed in bfloat16 or wider, within the bound.
A program may use at most 128 MiB of HBM per device.

```python
import math
import jax
import jax.numpy as jnp
from jax import lax

D = 3072
HEADS = 24
HD = 128
C = 64
TOK_DEV = 256
LIVE = 128
TOKENS = 8192


def activation_draw(key, salt):
    inner = jax.random.fold_in(key, salt)
    first, second = jax.random.split(inner, 2)
    base = jnp.clip(jax.random.normal(first, (2, TOKENS, D), jnp.float32), -6.0, 6.0)
    row_scale = jnp.exp(jax.random.uniform(second, (2, TOKENS, 1), jnp.float32, math.log(0.5), math.log(2.0)))
    return base * row_scale


def draw_block_input(key, part):
    return activation_draw(key, 101).astype(jnp.bfloat16)


def draw_cached_out(key, part):
    return activation_draw(key, 202).astype(jnp.bfloat16)


def pair_draw(key):
    inner = jax.random.fold_in(key, 303)
    parts = jax.random.split(inner, 2)
    width = HEADS * HD
    queries = jnp.clip(jax.random.normal(parts[0], (2, TOKENS, width), jnp.float32), -6.0, 6.0)
    keys_drawn = jnp.clip(jax.random.normal(parts[1], (2, TOKENS, width), jnp.float32), -6.0, 6.0)
    return (queries, keys_drawn)


def draw_query_proj(key, part):
    return pair_draw(key)[0].astype(jnp.bfloat16)


def draw_key_proj(key, part):
    return pair_draw(key)[1].astype(jnp.bfloat16)


def gain_draw(key, salt):
    inner = jax.random.fold_in(key, salt)
    return jnp.exp(jax.random.uniform(inner, (HD,), jnp.float32, 0.0, math.log(2.5)))


def draw_query_gain(key, part):
    return gain_draw(key, 404)


def draw_key_gain(key, part):
    return gain_draw(key, 505)


def draw_replay_mask(key, part):
    inner = jax.random.fold_in(key, 606)
    first, second, third = jax.random.split(inner, 3)
    blocks = TOKENS // TOK_DEV
    counts = jax.random.randint(first, (2, blocks), max(LIVE // 8, 1), LIVE // 2 + 1)
    fullest = jax.random.randint(second, (2,), 0, blocks)
    counts = jnp.where(jnp.arange(blocks)[None, :] == fullest[:, None], LIVE, counts)
    streams = jax.random.split(third, 2 * blocks)
    ranks = jax.vmap(lambda stream: jax.random.permutation(stream, TOK_DEV))(streams).reshape(2, blocks, TOK_DEV)
    marked = jnp.where(ranks < counts[:, :, None], 0, 1)
    return marked.reshape(2, TOKENS).astype(jnp.int32)


def shard_levels(stream_key, shape, shards, least, largest):
    factor_of = 1.0
    for position, blocks in shards:
        heights = jax.random.uniform(jax.random.fold_in(jax.random.fold_in(stream_key, 6), position), (blocks,), jnp.float32, least / len(shards), largest / len(shards))
        factor_of = factor_of * jnp.repeat(jnp.exp(heights), shape[position] // blocks).reshape((-1,) + (1,) * (len(shape) - 1 - position))
    return factor_of


def noise(rng, dims, deviation, reach, cuts=(), dtype=jnp.bfloat16):
    drawn = jax.random.normal(rng, dims, jnp.float32) * deviation
    if len(cuts) > 0:
        drawn = shard_levels(rng, dims, cuts, -0.22, 0.18) * drawn
    return jnp.clip(drawn, min=-reach, max=reach).astype(dtype)


def setup_inputs(seed: int = 0) -> dict:
    streams_of = jax.random.split(jax.random.key(seed), 14)
    query_proj = draw_query_proj(jax.random.fold_in(streams_of[13], 71), 0)
    key_proj = draw_key_proj(jax.random.fold_in(streams_of[13], 71), 0)
    value_proj = noise(streams_of[2], (2, TOKENS, HEADS * HD), 1.0, 6.0, ((0, 2), (1, 32), (2, 8)))
    query_gain = draw_query_gain(jax.random.fold_in(streams_of[13], 71), 0)
    key_gain = draw_key_gain(jax.random.fold_in(streams_of[13], 71), 0)
    block_input = draw_block_input(jax.random.fold_in(streams_of[13], 71), 0)
    cached_out = draw_cached_out(jax.random.fold_in(streams_of[13], 71), 0)
    replay_mask = draw_replay_mask(jax.random.fold_in(streams_of[13], 71), 0)
    branch_gate = jnp.clip(jnp.exp(math.log(4.0) - 1.3862944 * jax.random.uniform(streams_of[8], (2, D), jnp.float32) ** shard_levels(streams_of[8], (2, D), ((0, 2),), -0.2, 0.2)), 1.0, 4.0)
    attn_weight = noise(streams_of[9], (HEADS * HD, D), (HEADS * HD) ** -0.5, 0.109375, ((0, 8),))
    final_shift = noise(streams_of[10], (2, D), 1.0, 4.0, ((0, 2),), jnp.float32)
    final_scale = noise(streams_of[11], (2, D), 0.5, 2.0, ((0, 2),), jnp.float32)
    patch_weight = noise(streams_of[12], (D, C), D ** -0.5, 0.109375)
    return {"query_proj": query_proj, "key_proj": key_proj, "value_proj": value_proj, "query_gain": query_gain, "key_gain": key_gain, "block_input": block_input, "cached_out": cached_out, "replay_mask": replay_mask, "branch_gate": branch_gate, "attn_weight": attn_weight, "final_shift": final_shift, "final_scale": final_scale, "patch_weight": patch_weight}


def norm_heads(values, gain):
    lifted = values.astype(jnp.float32).reshape(values.shape[:-1] + (HEADS, HD))
    mean_square = lax.optimization_barrier(jnp.mean(lifted * lifted, axis=-1, keepdims=True))
    scaled = lifted * lax.rsqrt(mean_square + 1e-06) * gain
    return scaled.reshape(values.shape).astype(jnp.bfloat16)

def split_heads(values):
    return values.reshape(2, TOKENS, HEADS, HD).transpose(0, 2, 1, 3).reshape(2 * HEADS, TOKENS, HD)

def attend(queries, keys_normed, values_in):
    block = 1024 if TOKENS % 1024 == 0 else TOKENS
    scale = HD ** (-0.5)

    def one_head(triple):
        query_head, key_head, value_head = triple
        blocks = query_head.reshape(TOKENS // block, block, HD)

        def one_block(query_block):
            scores = jnp.dot(query_block, key_head.T, preferred_element_type=jnp.float32) * scale
            biggest = lax.optimization_barrier(jnp.max(scores, axis=-1, keepdims=True))
            weights = jnp.exp(scores - biggest)
            totals = lax.optimization_barrier(jnp.sum(weights, axis=-1, keepdims=True))
            summed = jnp.dot(weights.astype(jnp.bfloat16), value_head, preferred_element_type=jnp.float32)
            return (summed / totals).astype(jnp.bfloat16)
        return lax.map(one_block, blocks).reshape(TOKENS, HD)
    result = lax.map(one_head, (split_heads(queries), split_heads(keys_normed), split_heads(values_in)))
    return result.reshape(2, HEADS, TOKENS, HD).transpose(0, 2, 1, 3).reshape(2, TOKENS, HEADS * HD)

def reference(query_proj, key_proj, value_proj, query_gain, key_gain, block_input, cached_out, replay_mask, branch_gate, attn_weight, final_shift, final_scale, patch_weight):
    queries = norm_heads(query_proj, query_gain)
    keys_normed = norm_heads(key_proj, key_gain)
    attended = attend(queries, keys_normed, value_proj)
    outputs = []
    results = []
    for branch in range(2):
        projected = jnp.dot(attended[branch], attn_weight, preferred_element_type=jnp.float32)
        mixed = block_input[branch].astype(jnp.float32) + branch_gate[branch][None, :] * projected
        chosen = jnp.where(replay_mask[branch][:, None] == 1, cached_out[branch].astype(jnp.float32), mixed)
        block_out = chosen.astype(jnp.bfloat16)
        outputs.append(block_out)
        lifted = block_out.astype(jnp.float32)
        center = lax.optimization_barrier(jnp.mean(lifted, axis=-1, keepdims=True))
        spread = lax.optimization_barrier(jnp.mean((lifted - center) * (lifted - center), axis=-1, keepdims=True))
        normed = ((lifted - center) * lax.rsqrt(spread + 1e-06) * (1.0 + final_scale[branch][None, :]) + final_shift[branch][None, :]).astype(jnp.bfloat16)
        results.append(jnp.dot(normed, patch_weight, preferred_element_type=jnp.float32))
    velocity = results[1] + 3.0 * (results[0] - results[1])
    return (jnp.stack(outputs), velocity)
```

```python
import functools
import math

import jax
import jax.numpy as jnp
from jax import lax
from jax.experimental import pallas as pl
from jax.experimental.pallas import tpu as pltpu
from jax.sharding import PartitionSpec as P

guidance_scale = 3.0
f32 = jnp.float32
bf16 = jnp.bfloat16
cut = 512


def dot(a, b, contract=(1, 0)):
    return lax.dot_general(
        a, b, (((contract[0],), (contract[1],)), ((), ())), preferred_element_type=f32
    )


def remote(src, dst, sems, index, device):
    return pltpu.make_async_remote_copy(
        src_ref=src,
        dst_ref=dst,
        send_sem=sems[0].at[index],
        recv_sem=sems[1].at[index],
        device_id=device,
        device_id_type=pl.DeviceIdType.MESH,
    )


def kernel(
    ny,
    nz,
    q_ref,
    k_ref,
    v_ref,
    qg_ref,
    kg_ref,
    mask_ref,
    gate_ref,
    shift_ref,
    scale_ref,
    bi_hbm,
    co_hbm,
    w_hbm,
    pw_hbm,
    bo_hbm,
    vel_ref,
    bi_ref,
    co_ref,
    w_ref,
    pw_ref,
    bo_ref,
    sel_ref,
    kbuf,
    vbuf,
    rk,
    rv,
    qbuf,
    oacc,
    stat,
    own_o,
    own_s,
    osnd,
    orcv,
    att_ref,
    pbuf,
    zsnd,
    zrcv,
    ysnd,
    yrcv,
    loc_sem,
    qs,
    qr,
    ks,
    kr,
    os_,
    or_,
    zs,
    zr,
    ys,
    yr,
):
    count, width = q_ref.shape
    depth = qg_ref.shape[1]
    heads = width // depth
    live = qbuf.shape[3]
    share, feats = bi_ref.shape
    cuts = feats // cut
    c2 = depth ** (-0.5) * math.log2(math.e)
    yh, zh = ny // 2, nz // 2

    cfg = lax.axis_index("cfg")
    ctx = lax.axis_index("ctx")
    tp = lax.axis_index("tp")
    core = lax.rem(ctx, 2)
    hi = lax.rem(lax.div(ctx, 2), 2)
    y = lax.div(ctx, 4)
    x = hi * 2 + cfg

    def at_x(place):
        return {"cfg": lax.rem(place, 2), "ctx": y * 4 + lax.div(place, 2) * 2 + core}

    x_up, x_dn = at_x(lax.rem(x + 1, 4)), at_x(lax.rem(x + 3, 4))
    sib = {"ctx": ctx + 1 - 2 * core}
    y_up = {"ctx": lax.rem(y + 1, ny) * 4 + hi * 2 + core}
    y_dn = {"ctx": lax.rem(y + ny - 1, ny) * 4 + hi * 2 + core}
    z_up = {"tp": lax.rem(tp + 1, nz)}
    z_dn = {"tp": lax.rem(tp + nz - 1, nz)}
    other = {"cfg": 1 - cfg}

    barrier = pltpu.get_barrier_semaphore()
    for device in (x_up, x_dn, sib, y_up, y_dn, z_up, z_dn):
        pl.semaphore_signal(
            barrier, inc=1, device_id=device, device_id_type=pl.DeviceIdType.MESH
        )

    loads = [
        pltpu.make_async_copy(src, dst, loc_sem.at[n])
        for n, (src, dst) in enumerate(
            ((w_hbm, w_ref), (bi_hbm, bi_ref), (co_hbm, co_ref), (pw_hbm, pw_ref))
        )
    ]
    for load in loads:
        load.start()

    def q_up(s, h):
        return remote(
            qbuf.at[lax.rem(ny - s, ny), h], qbuf.at[ny - 1 - s, h], (qs, qr), (0, s, h), y_up
        )

    def q_dn(s, h):
        return remote(qbuf.at[s, h], qbuf.at[s + 1, h], (qs, qr), (1, s, h), y_dn)

    kv = (ks, kr)

    def k_sib(h):
        return remote(kbuf.at[0, h], kbuf.at[1, h], kv, (0, h), sib)

    def v_sib(h):
        return remote(vbuf.at[0, h], vbuf.at[1, h], kv, (1, h), sib)

    def k_out(h):
        return remote(kbuf.at[0, h], rk.at[h], kv, (2, h), x_up)

    def v_out(h):
        return remote(vbuf.at[0, h], rv.at[h], kv, (3, h), x_dn)

    def k_on(h):
        return remote(rk.at[h], kbuf.at[2, h], kv, (4, h), x_up)

    def v_on(h):
        return remote(rv.at[h], vbuf.at[2, h], kv, (5, h), x_dn)

    def k_last(h):
        return remote(kbuf.at[2, h], kbuf.at[3, h], kv, (6, h), sib)

    def v_last(h):
        return remote(vbuf.at[2, h], vbuf.at[3, h], kv, (7, h), sib)

    def o_up(s, h):
        return remote(osnd.at[0, s, h], orcv.at[0, s, h], (os_, or_), (0, s, h), y_up)

    def o_dn(s, h):
        return remote(osnd.at[1, s, h], orcv.at[1, s, h], (os_, or_), (1, s, h), y_dn)

    def z_upc(s, n):
        return remote(zsnd.at[0, s, n], zrcv.at[0, s, n], (zs, zr), (0, s, n), z_up)

    def z_dnc(s, n):
        return remote(zsnd.at[1, s, n], zrcv.at[1, s, n], (zs, zr), (1, s, n), z_dn)

    alive = (mask_ref[...] == 0).astype(f32)
    alive8 = jnp.broadcast_to(alive, (8, count))
    before = (
        lax.broadcasted_iota(jnp.int32, (count, count), 0)
        < lax.broadcasted_iota(jnp.int32, (count, count), 1)
    ).astype(f32)
    rank = dot(alive8.astype(bf16), before.astype(bf16))[0:1]
    slot = lax.broadcasted_iota(jnp.int32, (live, count), 0).astype(f32)
    picks = jnp.where((slot == rank) & (alive > 0.5), 1.0, 0.0)
    sel_ref[...] = picks.T.astype(bf16)
    picks = picks.astype(bf16)

    def normed_head(ref, gain_ref, h):
        part = ref[:, h * depth : (h + 1) * depth].astype(f32)
        square = jnp.mean(part * part, axis=-1, keepdims=True)
        return part * lax.rsqrt(square + 1e-06) * gain_ref[...]

    for h in range(heads):
        qn = normed_head(q_ref, qg_ref, h).astype(bf16)
        qbuf[0, h] = dot(picks, qn).T.astype(bf16)
        kbuf[0, h] = normed_head(k_ref, kg_ref, h).astype(bf16)
        vbuf[0, h] = v_ref[:, h * depth : (h + 1) * depth].astype(f32).T.astype(bf16)
        if h == 0:
            pl.semaphore_wait(barrier, 7)
        k_out(h).start()
        v_out(h).start()
        q_up(0, h).start()
        q_dn(0, h).start()
        k_sib(h).start()
        v_sib(h).start()

    def half(h, a, b, first):
        pair = (0, 1) if first else (2, 3)
        q2 = jnp.concatenate([qbuf[a, h], qbuf[b, h]], axis=1)
        scores = [dot(kbuf[j, h], q2) for j in pair]
        top = jnp.maximum(*[jnp.max(s, axis=0, keepdims=True) for s in scores])
        top = top.astype(bf16).astype(f32)
        if not first:
            old = jnp.concatenate([stat[a, h, 0:1], stat[b, h, 0:1]], axis=1)
            top = jnp.maximum(top, old)
        weights = [jnp.exp2((s - top) * c2) for s in scores]
        total = sum(jnp.sum(w, axis=0, keepdims=True) for w in weights)
        summed = sum(dot(vbuf[j, h], w.astype(bf16)) for j, w in zip(pair, weights))
        if not first:
            factor = jnp.exp2((old - top) * c2)
            total += factor * jnp.concatenate([stat[a, h, 1:2], stat[b, h, 1:2]], axis=1)
            summed += factor * jnp.concatenate([oacc[a, h], oacc[b, h]], axis=1)
        return summed, top, total

    def q_step(s, carry):
        a, b = ny - 1 - s, lax.rem(s + 1, yh)
        for h in range(heads):
            q_up(s, h).wait_recv()

            @pl.when(s < yh - 1)
            def _():
                q_up(s + 1, h).start()
                q_dn(s, h).wait_recv()

            @pl.when(s < yh - 2)
            def _():
                q_dn(s + 1, h).start()

            @pl.when(s == 0)
            def _():
                k_out(h).wait_recv()
                k_on(h).start()
                v_out(h).wait_recv()
                v_on(h).start()
                k_sib(h).wait_recv()
                v_sib(h).wait_recv()

            @pl.when(s == 1)
            def _():
                k_on(h).wait_recv()
                k_last(h).start()
                v_on(h).wait_recv()
                v_last(h).start()

            summed, top, total = half(h, a, b, True)
            for n, place in enumerate((a, b)):
                lanes = slice(n * live, (n + 1) * live)
                oacc[place, h] = summed[:, lanes]
                stat[place, h, 0:1] = top[:, lanes]
                stat[place, h, 1:2] = total[:, lanes]
        return carry

    lax.fori_loop(0, yh, q_step, 0)

    for h in range(heads):
        k_last(h).wait_recv()
        v_last(h).wait_recv()

    def put(way, s, h, summed, top, total):
        osnd[way, s, h, 0:depth] = summed.astype(bf16)
        high = total.astype(bf16).astype(f32)
        row = lax.broadcasted_iota(jnp.int32, (16, live), 0)
        tile = jnp.where(row == 0, top, jnp.where(row == 1, high, total - high))
        osnd[way, s, h, depth : depth + 16] = tile.astype(bf16)

    def merge(way, s, h, summed, top, total):
        theirs = orcv[way, s, h, 0:depth].astype(f32)
        tile = orcv[way, s, h, depth : depth + 16].astype(f32)
        their_top, their_total = tile[0:1], tile[1:2] + tile[2:3]
        newest = jnp.maximum(top, their_top)
        mine, factor = jnp.exp2((top - newest) * c2), jnp.exp2((their_top - newest) * c2)
        return summed * mine + theirs * factor, newest, total * mine + their_total * factor

    def split(parts, n):
        return [part[:, n * live : (n + 1) * live] for part in parts]

    for h in range(heads):
        parts = half(h, yh, yh + 1, False)
        put(0, 0, h, *split(parts, 0))
        o_up(0, h).start()
        put(1, 0, h, *split(parts, 1))
        o_dn(0, h).start()

    def o_step(s, carry):
        for h in range(heads):
            parts = half(h, yh - s, lax.rem(yh + 1 + s, ny), False)
            o_up(s - 1, h).wait_recv()
            put(0, s, h, *merge(0, s - 1, h, *split(parts, 0)))
            o_up(s, h).start()
            o_dn(s - 1, h).wait_recv()
            summed, top, total = merge(1, s - 1, h, *split(parts, 1))

            @pl.when(s < yh - 1)
            def _():
                put(1, s, h, summed, top, total)
                o_dn(s, h).start()

            own_o[h] = summed
            own_s[h, 0:1] = top
            own_s[h, 1:2] = total
        return carry

    lax.fori_loop(1, yh, o_step, 0)

    for h in range(heads):
        o_up(yh - 1, h).wait_recv()
        summed, top, total = merge(0, yh - 1, h, own_o[h], own_s[h, 0:1], own_s[h, 1:2])
        done = (summed / total).astype(bf16)
        att_ref[:, h * depth : (h + 1) * depth] = dot(sel_ref[...], done, (1, 1)).astype(bf16)

    loads[0].wait()

    def rows_of(n, place):
        start = pl.multiple_of(place * share, share)
        return pbuf[n, pl.ds(start, share), :]

    def z_first(n, carry):
        columns = pl.ds(pl.multiple_of(n * cut, cut), cut)
        pbuf[n] = dot(att_ref[...], w_ref[:, columns])
        zsnd[0, 0, n] = rows_of(n, lax.rem(tp + zh, nz)).astype(bf16)
        z_upc(0, n).start()
        zsnd[1, 0, n] = rows_of(n, lax.rem(tp + zh + 1, nz)).astype(bf16)
        z_dnc(0, n).start()
        return carry

    lax.fori_loop(0, cuts, z_first, 0)

    def z_step(s, carry):
        def z_cut(n, inner):
            z_upc(s - 1, n).wait_recv()
            part = rows_of(n, lax.rem(tp + zh - s, nz))
            zsnd[0, s, n] = (part + zrcv[0, s - 1, n].astype(f32)).astype(bf16)
            z_upc(s, n).start()

            @pl.when(s < zh - 1)
            def _():
                z_dnc(s - 1, n).wait_recv()
                part = rows_of(n, lax.rem(tp + zh + 1 + s, nz))
                zsnd[1, s, n] = (part + zrcv[1, s - 1, n].astype(f32)).astype(bf16)
                z_dnc(s, n).start()

            return inner

        return lax.fori_loop(0, cuts, z_cut, carry)

    lax.fori_loop(1, zh, z_step, 0)

    loads[1].wait()
    loads[2].wait()
    loads[3].wait()
    own_rows = pl.ds(pl.multiple_of(tp * share, share), share)
    alive_rows = jnp.sum(sel_ref[own_rows, :].astype(f32), axis=1, keepdims=True) > 0.5
    sums = jnp.zeros((share, 1), f32)
    for n in range(cuts):
        columns = slice(n * cut, (n + 1) * cut)
        z_upc(zh - 1, n).wait_recv()
        z_dnc(zh - 2, n).wait_recv()
        projected = (
            rows_of(n, tp) + zrcv[0, zh - 1, n].astype(f32) + zrcv[1, zh - 2, n].astype(f32)
        )
        mixed = bi_ref[:, columns].astype(f32) + gate_ref[:, columns] * projected
        out = jnp.where(alive_rows, mixed, co_ref[:, columns].astype(f32)).astype(bf16)
        bo_ref[:, columns] = out
        sums += jnp.sum(out.astype(f32), axis=1, keepdims=True)
    store = pltpu.make_async_copy(bo_ref, bo_hbm, loc_sem.at[4])
    store.start()
    center = sums * (1.0 / feats)
    away = bo_ref[...].astype(f32) - center
    spread = jnp.mean(away * away, axis=1, keepdims=True)
    normed = away * lax.rsqrt(spread + 1e-06) * (1.0 + scale_ref[...]) + shift_ref[...]
    ysnd[...] = dot(normed.astype(bf16), pw_ref[...], (1, 1))
    swap = remote(ysnd, yrcv, (ys, yr), 0, other)
    swap.start()
    swap.wait_recv()
    mine, theirs = ysnd[...], yrcv[...]
    cond = jnp.where(cfg == 0, mine, theirs)
    uncond = jnp.where(cfg == 0, theirs, mine)
    velocity = uncond + guidance_scale * (cond - uncond)
    half_width = vel_ref.shape[1]
    vel_ref[...] = jnp.where(cfg == 0, velocity[:, :half_width], velocity[:, half_width:])

    store.wait()
    swap.wait_send()
    for h in range(heads):
        for copy in (k_sib, v_sib, k_out, v_out, k_on, v_on, k_last, v_last):
            copy(h).wait_send()

    def drain(s, carry):
        for h in range(heads):
            q_up(s, h).wait_send()
            o_up(s, h).wait_send()

            @pl.when(s < yh - 1)
            def _():
                q_dn(s, h).wait_send()
                o_dn(s, h).wait_send()

        return carry

    lax.fori_loop(0, yh, drain, 0)

    def z_drain(s, carry):
        def one(n, inner):
            z_upc(s, n).wait_send()

            @pl.when(s < zh - 1)
            def _():
                z_dnc(s, n).wait_send()

            return inner

        return lax.fori_loop(0, cuts, one, carry)

    lax.fori_loop(0, zh, z_drain, 0)


def shards(
    query_proj,
    key_proj,
    value_proj,
    query_gain,
    key_gain,
    block_input,
    cached_out,
    replay_mask,
    branch_gate,
    attn_weight,
    final_shift,
    final_scale,
    patch_weight,
):
    ny = lax.axis_size("ctx") // 4
    nz = lax.axis_size("tp")
    count, width = query_proj.shape[1:]
    depth = query_gain.shape[0]
    heads = width // depth
    live = count // 2
    share, feats = block_input.shape[1:]
    channels = patch_weight.shape[1]
    yh, zh = ny // 2, nz // 2
    cuts = feats // cut
    vmem = pl.BlockSpec(memory_space=pltpu.VMEM)
    anywhere = pl.BlockSpec(memory_space=pl.ANY)
    dma = pltpu.SemaphoreType.DMA
    block_out, velocity = pl.pallas_call(
        functools.partial(kernel, ny, nz),
        out_shape=(
            jax.ShapeDtypeStruct((share, feats), bf16),
            jax.ShapeDtypeStruct((share, channels // 2), f32),
        ),
        in_specs=[vmem] * 9 + [anywhere] * 4,
        out_specs=(anywhere, vmem),
        scratch_shapes=[
            pltpu.VMEM((share, feats), bf16),
            pltpu.VMEM((share, feats), bf16),
            pltpu.VMEM((width, feats), bf16),
            pltpu.VMEM((channels, feats), bf16),
            pltpu.VMEM((share, feats), bf16),
            pltpu.VMEM((count, live), bf16),
            pltpu.VMEM((4, heads, count, depth), bf16),
            pltpu.VMEM((4, heads, depth, count), bf16),
            pltpu.VMEM((heads, count, depth), bf16),
            pltpu.VMEM((heads, depth, count), bf16),
            pltpu.VMEM((ny, heads, depth, live), bf16),
            pltpu.VMEM((ny, heads, depth, live), f32),
            pltpu.VMEM((ny, heads, 8, live), f32),
            pltpu.VMEM((heads, depth, live), f32),
            pltpu.VMEM((heads, 8, live), f32),
            pltpu.VMEM((2, yh, heads, depth + 16, live), bf16),
            pltpu.VMEM((2, yh, heads, depth + 16, live), bf16),
            pltpu.VMEM((count, width), bf16),
            pltpu.VMEM((cuts, count, cut), f32),
            pltpu.VMEM((2, zh, cuts, share, cut), bf16),
            pltpu.VMEM((2, zh, cuts, share, cut), bf16),
            pltpu.VMEM((share, channels), f32),
            pltpu.VMEM((share, channels), f32),
            dma((5,)),
            dma((2, yh, heads)),
            dma((2, yh, heads)),
            dma((8, heads)),
            dma((8, heads)),
            dma((2, yh, heads)),
            dma((2, yh, heads)),
            dma((2, zh, cuts)),
            dma((2, zh, cuts)),
            dma((1,)),
            dma((1,)),
        ],
        compiler_params=pltpu.CompilerParams(
            collective_id=0, has_side_effects=True, vmem_limit_bytes=56 * 1024 * 1024
        ),
        name="block",
    )(
        query_proj[0],
        key_proj[0],
        value_proj[0],
        query_gain[None],
        key_gain[None],
        replay_mask,
        branch_gate,
        final_shift,
        final_scale,
        block_input[0],
        cached_out[0],
        attn_weight,
        patch_weight.T,
    )
    return (block_out[None], velocity)


def solution(mesh):
    in_specs = (
        P("cfg", "ctx", "tp"),
        P("cfg", "ctx", "tp"),
        P("cfg", "ctx", "tp"),
        P(),
        P(),
        P("cfg", ("ctx", "tp"), None),
        P("cfg", ("ctx", "tp"), None),
        P("cfg", "ctx"),
        P("cfg", None),
        P("tp", None),
        P("cfg", None),
        P("cfg", None),
        P(),
    )
    out_specs = (P("cfg", ("ctx", "tp"), None), P(("ctx", "tp"), "cfg"))
    return jax.shard_map(shards, mesh=mesh, in_specs=in_specs, out_specs=out_specs, check_vma=False)
```

```python
import functools
import math

import jax
import jax.numpy as jnp
from jax import lax
from jax.experimental import pallas as pl
from jax.experimental.pallas import tpu as pltpu
from jax.sharding import PartitionSpec as P

guidance_scale = 3.0
f32 = jnp.float32
bf16 = jnp.bfloat16
cut = 512


def dot(a, b, contract=(1, 0)):
    return lax.dot_general(
        a, b, (((contract[0],), (contract[1],)), ((), ())), preferred_element_type=f32
    )


def remote(src, dst, sems, kind, index, device):
    return pltpu.make_async_remote_copy(
        src_ref=src,
        dst_ref=dst,
        send_sem=sems[0].at[kind],
        recv_sem=sems[1].at[index],
        device_id=device,
        device_id_type=pl.DeviceIdType.MESH,
    )


def kernel(
    ny,
    nz,
    q_hbm,
    k_hbm,
    v_hbm,
    qg_hbm,
    kg_hbm,
    mask_hbm,
    gate_hbm,
    shift_hbm,
    scale_hbm,
    bi_hbm,
    co_hbm,
    w_hbm,
    pw_hbm,
    bo_out,
    vel_out,
    bo_ref,
    vel_ref,
    q_ref,
    k_ref,
    v_ref,
    qg_ref,
    kg_ref,
    mask_ref,
    gate_ref,
    shift_ref,
    scale_ref,
    bi_ref,
    co_ref,
    w_ref,
    pw_ref,
    sel_ref,
    kbuf,
    vbuf,
    rk,
    rv,
    qbuf,
    oacc,
    stat,
    part_o,
    part_s,
    own_o,
    own_s,
    osnd,
    orcv,
    att_ref,
    pbuf,
    zsnd,
    zrcv,
    ysnd,
    yrcv,
    loc_sem,
    left,
    qr,
    kr,
    or_,
    zr,
    yr,
):
    count, width = q_ref.shape
    depth = qg_ref.shape[1]
    heads = width // depth
    live = qbuf.shape[3]
    share, feats = bi_ref.shape
    cuts = feats // cut
    c2 = depth ** (-0.5) * math.log2(math.e)
    yh, zh = ny // 2, nz // 2

    cfg = lax.axis_index("cfg")
    ctx = lax.axis_index("ctx")
    tp = lax.axis_index("tp")
    core = lax.rem(ctx, 2)
    hi = lax.rem(lax.div(ctx, 2), 2)
    y = lax.div(ctx, 4)
    x = hi * 2 + cfg

    def at_x(place):
        return {"cfg": lax.rem(place, 2), "ctx": y * 4 + lax.div(place, 2) * 2 + 1 - core}

    x_up, x_dn = at_x(lax.rem(x + 1, 4)), at_x(lax.rem(x + 3, 4))
    sib = {"ctx": ctx + 1 - 2 * core}
    y_up = {"ctx": lax.rem(y + 1, ny) * 4 + hi * 2 + 1 - core}
    y_dn = {"ctx": lax.rem(y + ny - 1, ny) * 4 + hi * 2 + 1 - core}
    z_up = {"tp": lax.rem(tp + 1, nz)}
    z_dn = {"tp": lax.rem(tp + nz - 1, nz)}
    other = {"cfg": 1 - cfg}

    barrier = pltpu.get_barrier_semaphore()
    for device in (x_up, x_dn, sib, y_up, y_dn, z_up, z_dn, other):
        pl.semaphore_signal(
            barrier, inc=1, device_id=device, device_id_type=pl.DeviceIdType.MESH
        )

    pairs = (
        (mask_hbm, mask_ref),
        (q_hbm, q_ref),
        (qg_hbm, qg_ref),
        (k_hbm, k_ref),
        (kg_hbm, kg_ref),
        (v_hbm, v_ref),
        (w_hbm, w_ref),
        (bi_hbm, bi_ref),
        (co_hbm, co_ref),
        (gate_hbm, gate_ref),
        (scale_hbm, scale_ref),
        (shift_hbm, shift_ref),
        (pw_hbm, pw_ref),
    )
    loads = [
        pltpu.make_async_copy(src, dst, loc_sem.at[n]) for n, (src, dst) in enumerate(pairs)
    ]
    for load in loads:
        load.start()

    def q_up(s, h):
        return remote(
            qbuf.at[lax.rem(ny - s, ny), h], qbuf.at[ny - 1 - s, h], (left, qr), 0, (s, h), y_up
        )

    def q_dn(s, h):
        return remote(qbuf.at[s, h], qbuf.at[s + 1, h], (left, qr), 0, (yh + s, h), y_dn)

    kv = (left, kr)
    first_leg, second_leg = heads, 2 * heads

    def k_sib(h):
        return remote(kbuf.at[0, h], kbuf.at[1, h], kv, 1, 0, sib)

    def v_sib(h):
        return remote(vbuf.at[0, h], vbuf.at[1, h], kv, 2, 0, sib)

    def k_out(h):
        return remote(kbuf.at[0, h], rk.at[h], kv, 1, first_leg + h, x_up)

    def v_out(h):
        return remote(vbuf.at[0, h], rv.at[h], kv, 2, first_leg + h, x_dn)

    def k_on(h):
        return remote(rk.at[h], kbuf.at[2, h], kv, 1, second_leg + h, x_up)

    def v_on(h):
        return remote(rv.at[h], vbuf.at[2, h], kv, 2, second_leg + h, x_dn)

    def k_last(h):
        return remote(kbuf.at[2, h], kbuf.at[3, h], kv, 1, 1, sib)

    def v_last(h):
        return remote(vbuf.at[2, h], vbuf.at[3, h], kv, 2, 1, sib)

    def kv_come(n, index):
        block = kbuf.at[0, 0:2] if n == 1 else kbuf.at[0:2]
        remote(block, block, kv, 1, index, sib).wait_recv()

    def o_up(s, h):
        return remote(osnd.at[s, h], orcv.at[s, h], (left, or_), 3, (s, h), y_up)

    def o_dn(s, h):
        return remote(
            osnd.at[yh + s, h], orcv.at[yh + s, h], (left, or_), 3, (yh + s, h), y_dn
        )

    def z_upc(s, n):
        return remote(zsnd.at[s, n], zrcv.at[s, n], (left, zr), 4, (s, n), z_up)

    def z_dnc(s, n):
        place = nz - 2 - s
        return remote(zsnd.at[place, n], zrcv.at[place, n], (left, zr), 4, (place, n), z_dn)

    loads[0].wait()
    alive = (mask_ref[...] == 0).astype(f32)
    alive8 = jnp.broadcast_to(alive, (8, count))
    before = (
        lax.broadcasted_iota(jnp.int32, (count, count), 0)
        < lax.broadcasted_iota(jnp.int32, (count, count), 1)
    ).astype(f32)
    rank = dot(alive8.astype(bf16), before.astype(bf16))[0:1]
    slot = lax.broadcasted_iota(jnp.int32, (live, count), 0).astype(f32)
    picks = jnp.where((slot == rank) & (alive > 0.5), 1.0, 0.0)
    sel_ref[...] = picks.T.astype(bf16)
    picks = picks.astype(bf16)

    def normed_head(ref, gain_ref, h):
        part = ref[:, h * depth : (h + 1) * depth].astype(f32)
        square = jnp.mean(part * part, axis=-1, keepdims=True)
        return part * lax.rsqrt(square + 1e-06) * gain_ref[...]

    for load in loads[1:3]:
        load.wait()
    for h in range(heads):
        qn = normed_head(q_ref, qg_ref, h).astype(bf16)
        qbuf[0, h] = dot(picks, qn).T.astype(bf16)
        if h == 0:
            pl.semaphore_wait(barrier, 8)
        q_up(0, h).start()
        q_dn(0, h).start()
    for load in loads[3:6]:
        load.wait()
    for h in range(heads):
        kbuf[0, h] = normed_head(k_ref, kg_ref, h).astype(bf16)
        k_out(h).start()
        vbuf[0, h] = v_ref[:, h * depth : (h + 1) * depth].astype(f32).T.astype(bf16)
        v_out(h).start()
        k_sib(h).start()
        v_sib(h).start()

    def lanes(ref, a, b, *index):
        return jnp.concatenate([ref[(a, *index)], ref[(b, *index)]], axis=1)

    def halves(a, b, first):
        pair = (0, 1) if first else (2, 3)

        def scores_of(h):
            q2 = lanes(qbuf, a, b, h)
            return [dot(kbuf[j, h], q2) for j in pair]

        ahead = scores_of(0)
        for h in range(heads):
            scores = ahead
            if h + 1 < heads:
                ahead = scores_of(h + 1)
            top = jnp.maximum(*[jnp.max(s, axis=0, keepdims=True) for s in scores])
            top = top.astype(bf16).astype(f32)
            if not first:
                old = lanes(stat, a, b, h, slice(0, 1))
                top = jnp.maximum(top, old)
            weights = [jnp.exp2((s - top) * c2) for s in scores]
            total = sum(jnp.sum(w, axis=0, keepdims=True) for w in weights)
            summed = sum(dot(vbuf[j, h], w.astype(bf16)) for j, w in zip(pair, weights))
            if not first:
                factor = jnp.exp2((old - top) * c2)
                total += factor * lanes(stat, a, b, h, slice(1, 2))
                summed += factor * lanes(oacc, a, b, h)
            yield summed, top, total

    def near(a, b):
        for h, (summed, top, total) in enumerate(halves(a, b, True)):
            for n, place in enumerate((a, b)):
                part = slice(n * live, (n + 1) * live)
                oacc[place, h] = summed[:, part]
                stat[place, h, 0:1] = top[:, part]
                stat[place, h, 1:2] = total[:, part]

    def relay(g):
        kv_come(1, first_leg + g)
        k_on(g).start()
        v_on(g).start()

    def last_leg(g):
        kv_come(1, second_leg + g)
        k_last(g).start()
        v_last(g).start()

    def q_pass(s):
        for h in range(heads):
            q_up(s, h).wait_recv()
            q_up(s + 1, h).start()
            q_dn(s, h).wait_recv()

            @pl.when(s < yh - 2)
            def _():
                q_dn(s + 1, h).start()

    def q_step(s, carry):
        @pl.when(s == 1)
        def _():
            relay(1)

        q_pass(s)

        @pl.when(s == 0)
        def _():
            kv_come(heads, 0)
            relay(0)

        @pl.when(s == 1)
        def _():
            relay(2)

        @pl.when(s == 2)
        def _():
            last_leg(0)
            last_leg(1)

        near(ny - 1 - s, s + 1)
        return carry

    lax.fori_loop(0, yh - 1, q_step, 0)
    last_leg(2)
    for h in range(heads):
        q_up(yh - 1, h).wait_recv()
    near(yh, 0)
    kv_come(heads, 1)

    def put(way, s, h, summed, top, total):
        osnd[way * yh + s, h, 0:depth] = summed.astype(bf16)
        high = total.astype(bf16).astype(f32)
        row = lax.broadcasted_iota(jnp.int32, (16, live), 0)
        tile = jnp.where(row == 0, top, jnp.where(row == 1, high, total - high))
        osnd[way * yh + s, h, depth : depth + 16] = tile.astype(bf16)

    def merge(way, s, h, summed, top, total):
        theirs = orcv[way * yh + s, h, 0:depth].astype(f32)
        tile = orcv[way * yh + s, h, depth : depth + 16].astype(f32)
        their_top, their_total = tile[0:1], tile[1:2] + tile[2:3]
        newest = jnp.maximum(top, their_top)
        mine, factor = jnp.exp2((top - newest) * c2), jnp.exp2((their_top - newest) * c2)
        return summed * mine + theirs * factor, newest, total * mine + their_total * factor

    def split(parts, n):
        return [part[:, n * live : (n + 1) * live] for part in parts]

    for h, parts in enumerate(halves(yh, yh + 1, False)):
        put(0, 0, h, *split(parts, 0))
        o_up(0, h).start()
        put(1, 0, h, *split(parts, 1))
        o_dn(0, h).start()

    def o_step(s, carry):
        for h, (summed, top, total) in enumerate(halves(yh - s, lax.rem(yh + 1 + s, ny), False)):
            part_o[h] = summed
            part_s[h, 0:1] = top
            part_s[h, 1:2] = total
        for h in range(heads):
            parts = (part_o[h], part_s[h, 0:1], part_s[h, 1:2])
            o_up(s - 1, h).wait_recv()
            put(0, s, h, *merge(0, s - 1, h, *split(parts, 0)))
            o_up(s, h).start()
            o_dn(s - 1, h).wait_recv()
            summed, top, total = merge(1, s - 1, h, *split(parts, 1))
            put(1, s, h, summed, top, total)

            @pl.when(s < yh - 1)
            def _():
                o_dn(s, h).start()

            own_o[h] = summed
            own_s[h, 0:1] = top
            own_s[h, 1:2] = total
        return carry

    lax.fori_loop(1, yh, o_step, 0)

    for h in range(heads):
        o_up(yh - 1, h).wait_recv()
        summed, top, total = merge(0, yh - 1, h, own_o[h], own_s[h, 0:1], own_s[h, 1:2])
        done = (summed / total).astype(bf16)
        att_ref[:, h * depth : (h + 1) * depth] = dot(sel_ref[...], done, (1, 1)).astype(bf16)

    loads[6].wait()

    def rows_of(n, place):
        start = pl.multiple_of(place * share, share)
        return pbuf[n, pl.ds(start, share), :]

    def hops(n):
        odd = lax.rem(n, 2)
        return zh - odd, zh - 1 + odd

    def z_first(n, carry):
        up, down = hops(n)
        columns = pl.ds(pl.multiple_of(n * cut, cut), cut)
        pbuf[n] = dot(att_ref[...], w_ref[:, columns])
        zsnd[0, n] = rows_of(n, lax.rem(tp + up, nz)).astype(bf16)
        z_upc(0, n).start()
        zsnd[nz - 2, n] = rows_of(n, lax.rem(tp + nz - down, nz)).astype(bf16)
        z_dnc(0, n).start()
        return carry

    lax.fori_loop(0, cuts, z_first, 0)

    def z_step(s, carry):
        def z_cut(n, inner):
            up, down = hops(n)

            @pl.when(s < up)
            def _():
                z_upc(s - 1, n).wait_recv()
                part = rows_of(n, lax.rem(tp + up - s, nz))
                zsnd[s, n] = (part + zrcv[s - 1, n].astype(f32)).astype(bf16)
                z_upc(s, n).start()

            @pl.when(s < down)
            def _():
                z_dnc(s - 1, n).wait_recv()
                part = rows_of(n, lax.rem(tp + nz - down + s, nz))
                zsnd[nz - 2 - s, n] = (part + zrcv[nz - 1 - s, n].astype(f32)).astype(bf16)
                z_dnc(s, n).start()

            return inner

        return lax.fori_loop(0, cuts, z_cut, carry)

    lax.fori_loop(1, zh, z_step, 0)

    for load in loads[7:]:
        load.wait()
    own_rows = pl.ds(pl.multiple_of(tp * share, share), share)
    alive_rows = jnp.sum(sel_ref[own_rows, :].astype(f32), axis=1, keepdims=True) > 0.5
    sums = jnp.zeros((share, 1), f32)
    for n in range(cuts):
        columns = slice(n * cut, (n + 1) * cut)
        up, down = zh - n % 2, zh - 1 + n % 2
        z_upc(up - 1, n).wait_recv()
        z_dnc(down - 1, n).wait_recv()
        projected = (
            rows_of(n, tp) + zrcv[up - 1, n].astype(f32) + zrcv[nz - 1 - down, n].astype(f32)
        )
        mixed = bi_ref[:, columns].astype(f32) + gate_ref[:, columns] * projected
        out = jnp.where(alive_rows, mixed, co_ref[:, columns].astype(f32)).astype(bf16)
        bo_ref[:, columns] = out
        sums += jnp.sum(out.astype(f32), axis=1, keepdims=True)
    store = pltpu.make_async_copy(bo_ref, bo_out, loc_sem.at[13])
    store.start()
    center = sums * (1.0 / feats)
    away = bo_ref[...].astype(f32) - center
    spread = jnp.mean(away * away, axis=1, keepdims=True)
    normed = away * lax.rsqrt(spread + 1e-06) * (1.0 + scale_ref[...]) + shift_ref[...]
    ysnd[...] = dot(normed.astype(bf16), pw_ref[...], (1, 1))
    swap = remote(ysnd, yrcv, (left, yr), 5, 0, other)
    swap.start()

    for kind, sent in enumerate(
        (qbuf.at[0 : ny - 1], kbuf, vbuf, osnd.at[0 : ny - 1], zsnd)
    ):
        remote(sent, sent, (left, qr), kind, (0, 0), sib).wait_send()
    swap.wait()
    mine, theirs = ysnd[...], yrcv[...]
    cond = jnp.where(cfg == 0, mine, theirs)
    uncond = jnp.where(cfg == 0, theirs, mine)
    velocity = uncond + guidance_scale * (cond - uncond)
    half_width = vel_ref.shape[1]
    vel_ref[...] = jnp.where(cfg == 0, velocity[:, :half_width], velocity[:, half_width:])
    last = pltpu.make_async_copy(vel_ref, vel_out, loc_sem.at[14])
    last.start()
    store.wait()
    last.wait()


def shards(
    query_proj,
    key_proj,
    value_proj,
    query_gain,
    key_gain,
    block_input,
    cached_out,
    replay_mask,
    branch_gate,
    attn_weight,
    final_shift,
    final_scale,
    patch_weight,
):
    ny = lax.axis_size("ctx") // 4
    nz = lax.axis_size("tp")
    count, width = query_proj.shape[1:]
    depth = query_gain.shape[0]
    heads = width // depth
    live = count // 2
    share, feats = block_input.shape[1:]
    channels = patch_weight.shape[1]
    yh, zh = ny // 2, nz // 2
    cuts = feats // cut
    anywhere = pl.BlockSpec(memory_space=pl.ANY)
    hbm = pl.BlockSpec(memory_space=pltpu.HBM)
    dma = pltpu.SemaphoreType.DMA
    operands = (
        query_proj[0],
        key_proj[0],
        value_proj[0],
        query_gain[None],
        key_gain[None],
        replay_mask,
        branch_gate,
        final_shift,
        final_scale,
        block_input[0],
        cached_out[0],
        attn_weight,
        patch_weight.T,
    )
    block_out, velocity = pl.pallas_call(
        functools.partial(kernel, ny, nz),
        out_shape=(
            jax.ShapeDtypeStruct((share, feats), bf16),
            jax.ShapeDtypeStruct((share, channels // 2), f32),
        ),
        in_specs=[hbm] * 13,
        out_specs=(anywhere, anywhere),
        scratch_shapes=[
            pltpu.VMEM((share, feats), bf16),
            pltpu.VMEM((share, channels // 2), f32),
            *[pltpu.VMEM((count, width), bf16)] * 3,
            *[pltpu.VMEM((1, depth), f32)] * 2,
            pltpu.VMEM((1, count), jnp.int32),
            *[pltpu.VMEM((1, feats), f32)] * 3,
            *[pltpu.VMEM((share, feats), bf16)] * 2,
            pltpu.VMEM((width, feats), bf16),
            pltpu.VMEM((channels, feats), bf16),
            pltpu.VMEM((count, live), bf16),
            pltpu.VMEM((4, heads, count, depth), bf16),
            pltpu.VMEM((4, heads, depth, count), bf16),
            pltpu.VMEM((heads, count, depth), bf16),
            pltpu.VMEM((heads, depth, count), bf16),
            pltpu.VMEM((ny, heads, depth, live), bf16),
            pltpu.VMEM((ny, heads, depth, live), f32),
            pltpu.VMEM((ny, heads, 8, live), f32),
            pltpu.VMEM((heads, depth, 2 * live), f32),
            pltpu.VMEM((heads, 8, 2 * live), f32),
            pltpu.VMEM((heads, depth, live), f32),
            pltpu.VMEM((heads, 8, live), f32),
            *[pltpu.VMEM((ny, heads, depth + 16, live), bf16)] * 2,
            pltpu.VMEM((count, width), bf16),
            pltpu.VMEM((cuts, count, cut), f32),
            *[pltpu.VMEM((nz - 1, cuts, share, cut), bf16)] * 2,
            pltpu.VMEM((share, channels), f32),
            pltpu.VMEM((share, channels), f32),
            dma((15,)),
            dma((6,)),
            dma((ny - 1, heads)),
            dma((3 * heads,)),
            dma((ny - 1, heads)),
            dma((nz - 1, cuts)),
            dma((1,)),
        ],
        compiler_params=pltpu.CompilerParams(
            collective_id=0, has_side_effects=True, vmem_limit_bytes=32 * 1024 * 1024
        ),
        name="block",
    )(*[pltpu.with_memory_space_constraint(operand, pltpu.HBM) for operand in operands])
    return (block_out[None], velocity)


def solution(mesh):
    in_specs = (
        P("cfg", "ctx", "tp"),
        P("cfg", "ctx", "tp"),
        P("cfg", "ctx", "tp"),
        P(),
        P(),
        P("cfg", ("ctx", "tp"), None),
        P("cfg", ("ctx", "tp"), None),
        P("cfg", "ctx"),
        P("cfg", None),
        P("tp", None),
        P("cfg", None),
        P("cfg", None),
        P(),
    )
    out_specs = (P("cfg", ("ctx", "tp"), None), P(("ctx", "tp"), "cfg"))
    return jax.shard_map(shards, mesh=mesh, in_specs=in_specs, out_specs=out_specs, check_vma=False)
```

```python
import functools
import math

import jax
import jax.numpy as jnp
from jax import lax
from jax.experimental import pallas as pl
from jax.experimental.pallas import tpu as pltpu
from jax.sharding import PartitionSpec as P

guidance_scale = 3.0
f32 = jnp.float32
bf16 = jnp.bfloat16
cut = 512


def dot(a, b, contract=(1, 0)):
    return lax.dot_general(
        a, b, (((contract[0],), (contract[1],)), ((), ())), preferred_element_type=f32
    )


def remote(src, dst, sems, kind, index, device):
    return pltpu.make_async_remote_copy(
        src_ref=src,
        dst_ref=dst,
        send_sem=sems[0].at[kind],
        recv_sem=sems[1].at[index],
        device_id=device,
        device_id_type=pl.DeviceIdType.MESH,
    )


def kernel(
    ny,
    nz,
    q_hbm,
    k_hbm,
    v_hbm,
    qg_hbm,
    kg_hbm,
    mask_hbm,
    gate_hbm,
    shift_hbm,
    scale_hbm,
    bi_hbm,
    co_hbm,
    w_hbm,
    pw_hbm,
    bo_out,
    vel_out,
    bo_ref,
    vel_ref,
    q_ref,
    k_ref,
    v_ref,
    qg_ref,
    kg_ref,
    mask_ref,
    gate_ref,
    shift_ref,
    scale_ref,
    bi_ref,
    co_ref,
    w_ref,
    pw_ref,
    sel_ref,
    kbuf,
    vbuf,
    rk,
    rv,
    qbuf,
    oacc,
    stat,
    part_o,
    part_s,
    own_o,
    own_s,
    osnd,
    orcv,
    att_ref,
    pbuf,
    zsnd,
    zrcv,
    ysnd,
    yrcv,
    loc_sem,
    left,
    qr,
    kr,
    or_,
    zr,
    yr,
):
    count, width = q_ref.shape
    depth = qg_ref.shape[1]
    heads = width // depth
    live = qbuf.shape[3]
    share, feats = bi_ref.shape
    cuts = feats // cut
    c2 = depth ** (-0.5) * math.log2(math.e)
    yh, zh = ny // 2, nz // 2

    cfg = lax.axis_index("cfg")
    ctx = lax.axis_index("ctx")
    tp = lax.axis_index("tp")
    core = lax.rem(ctx, 2)
    hi = lax.rem(lax.div(ctx, 2), 2)
    y = lax.div(ctx, 4)
    x = hi * 2 + cfg

    def at_x(place):
        return {"cfg": lax.rem(place, 2), "ctx": y * 4 + lax.div(place, 2) * 2 + 1 - core}

    x_up, x_dn = at_x(lax.rem(x + 1, 4)), at_x(lax.rem(x + 3, 4))
    sib = {"ctx": ctx + 1 - 2 * core}
    y_up = {"ctx": lax.rem(y + 1, ny) * 4 + hi * 2 + 1 - core}
    y_dn = {"ctx": lax.rem(y + ny - 1, ny) * 4 + hi * 2 + 1 - core}
    z_up = {"tp": lax.rem(tp + 1, nz)}
    z_dn = {"tp": lax.rem(tp + nz - 1, nz)}
    other = {"cfg": 1 - cfg}

    barrier = pltpu.get_barrier_semaphore()
    for device in (x_up, x_dn, sib, y_up, y_dn, z_up, z_dn, other):
        pl.semaphore_signal(
            barrier, inc=1, device_id=device, device_id_type=pl.DeviceIdType.MESH
        )

    pairs = (
        (mask_hbm, mask_ref),
        (q_hbm, q_ref),
        (qg_hbm, qg_ref),
        (k_hbm, k_ref),
        (kg_hbm, kg_ref),
        (v_hbm, v_ref),
        (w_hbm, w_ref),
        (bi_hbm, bi_ref),
        (co_hbm, co_ref),
        (gate_hbm, gate_ref),
        (scale_hbm, scale_ref),
        (shift_hbm, shift_ref),
        (pw_hbm, pw_ref),
    )
    loads = [
        pltpu.make_async_copy(src, dst, loc_sem.at[n]) for n, (src, dst) in enumerate(pairs)
    ]
    for load in loads:
        load.start()

    def q_up(s, h):
        return remote(
            qbuf.at[lax.rem(ny - s, ny), h], qbuf.at[ny - 1 - s, h], (left, qr), 0, (s, h), y_up
        )

    def q_dn(s, h):
        return remote(qbuf.at[s, h], qbuf.at[s + 1, h], (left, qr), 0, (yh + s, h), y_dn)

    kv = (left, kr)
    first_leg, second_leg, third_leg = 1, 1 + heads, 1 + 2 * heads

    def k_sib(h):
        return remote(kbuf.at[0, h], kbuf.at[1, h], kv, 1, 0, sib)

    def v_sib(h):
        return remote(vbuf.at[0, h], vbuf.at[1, h], kv, 2, 0, sib)

    def k_out(h):
        return remote(kbuf.at[0, h], rk.at[h], kv, 1, first_leg + h, x_up)

    def v_out(h):
        return remote(vbuf.at[0, h], rv.at[h], kv, 2, first_leg + h, x_dn)

    def k_on(h):
        return remote(rk.at[h], kbuf.at[2, h], kv, 1, second_leg + h, x_up)

    def v_on(h):
        return remote(rv.at[h], vbuf.at[2, h], kv, 2, second_leg + h, x_dn)

    def k_last(h):
        return remote(kbuf.at[2, h], kbuf.at[3, h], kv, 1, third_leg + h, sib)

    def v_last(h):
        return remote(vbuf.at[2, h], vbuf.at[3, h], kv, 2, third_leg + h, sib)

    def kv_come(n, index):
        block = kbuf.at[0, 0:2] if n == 1 else kbuf.at[0:2]
        remote(block, block, kv, 1, index, sib).wait_recv()

    def o_up(s, h):
        return remote(osnd.at[s, h], orcv.at[s, h], (left, or_), 3, (s, h), y_up)

    def o_dn(s, h):
        return remote(
            osnd.at[yh + s, h], orcv.at[yh + s, h], (left, or_), 3, (yh + s, h), y_dn
        )

    def z_upc(s, n):
        return remote(zsnd.at[s, n], zrcv.at[s, n], (left, zr), 4, (s, n), z_up)

    def z_dnc(s, n):
        place = nz - 2 - s
        return remote(zsnd.at[place, n], zrcv.at[place, n], (left, zr), 4, (place, n), z_dn)

    loads[0].wait()
    alive = (mask_ref[...] == 0).astype(f32)
    alive8 = jnp.broadcast_to(alive, (8, count))
    before = (
        lax.broadcasted_iota(jnp.int32, (count, count), 0)
        < lax.broadcasted_iota(jnp.int32, (count, count), 1)
    ).astype(f32)
    rank = dot(alive8.astype(bf16), before.astype(bf16))[0:1]
    slot = lax.broadcasted_iota(jnp.int32, (live, count), 0).astype(f32)
    picks = jnp.where((slot == rank) & (alive > 0.5), 1.0, 0.0)
    sel_ref[...] = picks.T.astype(bf16)
    picks = picks.astype(bf16)

    def normed_head(ref, gain_ref, h):
        part = ref[:, h * depth : (h + 1) * depth].astype(f32)
        square = jnp.mean(part * part, axis=-1, keepdims=True)
        return part * lax.rsqrt(square + 1e-06) * gain_ref[...]

    for load in loads[1:3]:
        load.wait()
    for h in range(heads):
        qn = normed_head(q_ref, qg_ref, h).astype(bf16)
        qbuf[0, h] = dot(picks, qn).T.astype(bf16)
    pl.semaphore_wait(barrier, 8)
    for h in range(heads):
        q_up(0, h).start()
        q_dn(0, h).start()
    for load in loads[3:6]:
        load.wait()
    for h in range(heads):
        kbuf[0, h] = normed_head(k_ref, kg_ref, h).astype(bf16)
        vbuf[0, h] = v_ref[:, h * depth : (h + 1) * depth].astype(f32).T.astype(bf16)
    for h in range(heads):
        k_out(h).start()
        v_out(h).start()
        k_sib(h).start()
        v_sib(h).start()

    def lanes(ref, places, *index):
        parts = [ref[(place, *index)] for place in places]
        return parts[0] if len(parts) == 1 else jnp.concatenate(parts, axis=1)

    def sums(places, slots, stored, which=range(heads)):
        def scores_of(h):
            queries = lanes(qbuf, places, h)
            return [dot(kbuf[j, h], queries) for j in slots]

        which = list(which)
        ahead = scores_of(which[0])
        for n, h in enumerate(which):
            scores = ahead
            if n + 1 < len(which):
                ahead = scores_of(which[n + 1])
            top = functools.reduce(
                jnp.maximum, [jnp.max(s, axis=0, keepdims=True) for s in scores]
            )
            top = top.astype(bf16).astype(f32)
            if stored:
                old = lanes(stat, places, h, slice(0, 1))
                top = jnp.maximum(top, old)
            weights = [jnp.exp2((s - top) * c2) for s in scores]
            total = sum(jnp.sum(w, axis=0, keepdims=True) for w in weights)
            summed = sum(dot(vbuf[j, h], w.astype(bf16)) for j, w in zip(slots, weights))
            if stored:
                factor = jnp.exp2((old - top) * c2)
                total += factor * lanes(stat, places, h, slice(1, 2))
                summed += factor * lanes(oacc, places, h)
            yield summed, top, total

    def near(*places):
        for h, (summed, top, total) in enumerate(sums(places, (0, 1), False)):
            for n, place in enumerate(places):
                part = slice(n * live, (n + 1) * live)
                oacc[place, h] = summed[:, part]
                stat[place, h, 0:1] = top[:, part]
                stat[place, h, 1:2] = total[:, part]

    def relay(g):
        kv_come(1, first_leg + g)
        k_on(g).start()
        v_on(g).start()

    def last_leg(g):
        kv_come(1, second_leg + g)
        k_last(g).start()
        v_last(g).start()

    def q_pass(s):
        for h in range(heads):
            q_up(s, h).wait_recv()
            q_up(s + 1, h).start()
            q_dn(s, h).wait_recv()

            @pl.when(s < yh - 2)
            def _():
                q_dn(s + 1, h).start()

            if h < heads - 1:

                @pl.when(s == yh - 2)
                def _():
                    last_leg(h)

    kv_come(heads, 0)
    near(0)

    def q_step(s, carry):
        @pl.when(s == 1)
        def _():
            relay(1)

        q_pass(s)

        @pl.when(s == 0)
        def _():
            relay(0)

        @pl.when(s == 1)
        def _():
            relay(2)

        near(ny - 1 - s, s + 1)
        return carry

    lax.fori_loop(0, yh - 1, q_step, 0)
    last_leg(2)

    def put(way, s, h, summed, top, total):
        osnd[way * yh + s, h, 0:depth] = summed.astype(bf16)
        high = total.astype(bf16).astype(f32)
        row = lax.broadcasted_iota(jnp.int32, (16, live), 0)
        tile = jnp.where(row == 0, top, jnp.where(row == 1, high, total - high))
        osnd[way * yh + s, h, depth : depth + 16] = tile.astype(bf16)

    def merge(way, s, h, summed, top, total):
        theirs = orcv[way * yh + s, h, 0:depth].astype(f32)
        tile = orcv[way * yh + s, h, depth : depth + 16].astype(f32)
        their_top, their_total = tile[0:1], tile[1:2] + tile[2:3]
        newest = jnp.maximum(top, their_top)
        mine, factor = jnp.exp2((top - newest) * c2), jnp.exp2((their_top - newest) * c2)
        return summed * mine + theirs * factor, newest, total * mine + their_total * factor

    for h in range(heads):
        q_up(yh - 1, h).wait_recv()
        kv_come(1, third_leg + h)
        for parts in sums((yh,), range(4), False, (h,)):
            put(0, 0, h, *parts)
            o_up(0, h).start()
    for h, parts in enumerate(sums((yh + 1,), (2, 3), True)):
        put(1, 0, h, *parts)
        o_dn(0, h).start()

    def own_sums(s):
        places = (yh - s, lax.rem(yh + 1 + s, ny))
        for h, (summed, top, total) in enumerate(sums(places, (2, 3), True)):
            part_o[lax.rem(s, 2), h] = summed
            part_s[lax.rem(s, 2), h, 0:1] = top
            part_s[lax.rem(s, 2), h, 1:2] = total

    def own_part(s, h, way):
        side = slice(way * live, (way + 1) * live)
        step = lax.rem(s, 2)
        return part_o[step, h, :, side], part_s[step, h, 0:1, side], part_s[step, h, 1:2, side]

    own_sums(1)

    def o_step(s, carry):
        for h in range(heads):
            o_up(s - 1, h).wait_recv()
            put(0, s, h, *merge(0, s - 1, h, *own_part(s, h, 0)))
            o_up(s, h).start()

        @pl.when(s < yh - 1)
        def _():
            own_sums(s + 1)

        for h in range(heads):
            o_dn(s - 1, h).wait_recv()
            below = merge(1, s - 1, h, *own_part(s, h, 1))

            @pl.when(s < yh - 1)
            def _():
                put(1, s, h, *below)
                o_dn(s, h).start()

            own_o[h], own_s[h, 0:1], own_s[h, 1:2] = below
        return carry

    lax.fori_loop(1, yh, o_step, 0)

    for h in range(heads):
        o_up(yh - 1, h).wait_recv()
        summed, top, total = merge(0, yh - 1, h, own_o[h], own_s[h, 0:1], own_s[h, 1:2])
        done = (summed / total).astype(bf16)
        att_ref[:, h * depth : (h + 1) * depth] = dot(sel_ref[...], done, (1, 1)).astype(bf16)

    loads[6].wait()

    def rows_of(n, place):
        start = pl.multiple_of(place * share, share)
        return pbuf[n, pl.ds(start, share), :]

    def hops(n):
        odd = lax.rem(n, 2)
        return zh - odd, zh - 1 + odd

    def z_first(n, carry):
        up, down = hops(n)
        columns = pl.ds(pl.multiple_of(n * cut, cut), cut)
        pbuf[n] = dot(att_ref[...], w_ref[:, columns])
        zsnd[0, n] = rows_of(n, lax.rem(tp + up, nz)).astype(bf16)
        z_upc(0, n).start()
        zsnd[nz - 2, n] = rows_of(n, lax.rem(tp + nz - down, nz)).astype(bf16)
        z_dnc(0, n).start()
        return carry

    lax.fori_loop(0, cuts, z_first, 0)

    def passed(place, n, dest):
        return rows_of(n, dest) + zrcv[place, n].astype(f32)

    def z_step(s, carry):
        def z_cut(n, inner):
            up, down = hops(n)
            z_upc(s - 1, n).wait_recv()
            z_dnc(s - 1, n).wait_recv()
            above = passed(s - 1, n, lax.rem(tp + up - s, nz))
            below = passed(nz - 1 - s, n, lax.rem(tp + nz - down + s, nz))
            zsnd[s, n] = above.astype(bf16)
            zsnd[nz - 2 - s, n] = below.astype(bf16)
            z_upc(s, n).start()
            z_dnc(s, n).start()
            return inner

        return lax.fori_loop(0, cuts, z_cut, carry)

    lax.fori_loop(1, zh - 1, z_step, 0)

    for n in range(cuts):
        if n % 2 == 0:
            z_upc(zh - 2, n).wait_recv()
            zsnd[zh - 1, n] = passed(zh - 2, n, lax.rem(tp + 1, nz)).astype(bf16)
            z_upc(zh - 1, n).start()
        else:
            z_dnc(zh - 2, n).wait_recv()
            zsnd[zh - 1, n] = passed(zh, n, lax.rem(tp + nz - 1, nz)).astype(bf16)
            z_dnc(zh - 1, n).start()

    for load in loads[7:]:
        load.wait()
    own_rows = pl.ds(pl.multiple_of(tp * share, share), share)
    alive_rows = jnp.sum(sel_ref[own_rows, :].astype(f32), axis=1, keepdims=True) > 0.5
    sums = jnp.zeros((share, 1), f32)
    for n in range(cuts):
        columns = slice(n * cut, (n + 1) * cut)
        up, down = zh - n % 2, zh - 1 + n % 2
        z_upc(up - 1, n).wait_recv()
        z_dnc(down - 1, n).wait_recv()
        projected = (
            rows_of(n, tp) + zrcv[up - 1, n].astype(f32) + zrcv[nz - 1 - down, n].astype(f32)
        )
        mixed = bi_ref[:, columns].astype(f32) + gate_ref[:, columns] * projected
        out = jnp.where(alive_rows, mixed, co_ref[:, columns].astype(f32)).astype(bf16)
        bo_ref[:, columns] = out
        sums += jnp.sum(out.astype(f32), axis=1, keepdims=True)
    store = pltpu.make_async_copy(bo_ref, bo_out, loc_sem.at[13])
    store.start()
    center = sums * (1.0 / feats)
    away = bo_ref[...].astype(f32) - center
    spread = jnp.mean(away * away, axis=1, keepdims=True)
    normed = away * lax.rsqrt(spread + 1e-06) * (1.0 + scale_ref[...]) + shift_ref[...]
    ysnd[...] = dot(normed.astype(bf16), pw_ref[...], (1, 1))
    swap = remote(ysnd, yrcv, (left, yr), 5, 0, other)
    swap.start()

    for kind, sent in enumerate(
        (qbuf.at[0 : ny - 1], kbuf, vbuf, osnd, zsnd)
    ):
        remote(sent, sent, (left, qr), kind, (0, 0), sib).wait_send()
    swap.wait()
    mine, theirs = ysnd[...], yrcv[...]
    cond = jnp.where(cfg == 0, mine, theirs)
    uncond = jnp.where(cfg == 0, theirs, mine)
    velocity = uncond + guidance_scale * (cond - uncond)
    half_width = vel_ref.shape[1]
    vel_ref[...] = jnp.where(cfg == 0, velocity[:, :half_width], velocity[:, half_width:])
    last = pltpu.make_async_copy(vel_ref, vel_out, loc_sem.at[14])
    last.start()
    store.wait()
    last.wait()


def shards(
    query_proj,
    key_proj,
    value_proj,
    query_gain,
    key_gain,
    block_input,
    cached_out,
    replay_mask,
    branch_gate,
    attn_weight,
    final_shift,
    final_scale,
    patch_weight,
):
    ny = lax.axis_size("ctx") // 4
    nz = lax.axis_size("tp")
    count, width = query_proj.shape[1:]
    depth = query_gain.shape[0]
    heads = width // depth
    live = count // 2
    share, feats = block_input.shape[1:]
    channels = patch_weight.shape[1]
    yh, zh = ny // 2, nz // 2
    cuts = feats // cut
    anywhere = pl.BlockSpec(memory_space=pl.ANY)
    hbm = pl.BlockSpec(memory_space=pltpu.HBM)
    dma = pltpu.SemaphoreType.DMA
    operands = (
        query_proj[0],
        key_proj[0],
        value_proj[0],
        query_gain[None],
        key_gain[None],
        replay_mask,
        branch_gate,
        final_shift,
        final_scale,
        block_input[0],
        cached_out[0],
        attn_weight,
        patch_weight.T,
    )
    block_out, velocity = pl.pallas_call(
        functools.partial(kernel, ny, nz),
        out_shape=(
            jax.ShapeDtypeStruct((share, feats), bf16),
            jax.ShapeDtypeStruct((share, channels // 2), f32),
        ),
        in_specs=[hbm] * 13,
        out_specs=(anywhere, anywhere),
        scratch_shapes=[
            pltpu.VMEM((share, feats), bf16),
            pltpu.VMEM((share, channels // 2), f32),
            *[pltpu.VMEM((count, width), bf16)] * 3,
            *[pltpu.VMEM((1, depth), f32)] * 2,
            pltpu.VMEM((1, count), jnp.int32),
            *[pltpu.VMEM((1, feats), f32)] * 3,
            *[pltpu.VMEM((share, feats), bf16)] * 2,
            pltpu.VMEM((width, feats), bf16),
            pltpu.VMEM((channels, feats), bf16),
            pltpu.VMEM((count, live), bf16),
            pltpu.VMEM((4, heads, count, depth), bf16),
            pltpu.VMEM((4, heads, depth, count), bf16),
            pltpu.VMEM((heads, count, depth), bf16),
            pltpu.VMEM((heads, depth, count), bf16),
            pltpu.VMEM((ny, heads, depth, live), bf16),
            pltpu.VMEM((ny, heads, depth, live), f32),
            pltpu.VMEM((ny, heads, 8, live), f32),
            pltpu.VMEM((2, heads, depth, 2 * live), f32),
            pltpu.VMEM((2, heads, 8, 2 * live), f32),
            pltpu.VMEM((heads, depth, live), f32),
            pltpu.VMEM((heads, 8, live), f32),
            *[pltpu.VMEM((ny - 1, heads, depth + 16, live), bf16)] * 2,
            pltpu.VMEM((count, width), bf16),
            pltpu.VMEM((cuts, count, cut), f32),
            *[pltpu.VMEM((nz - 1, cuts, share, cut), bf16)] * 2,
            pltpu.VMEM((share, channels), f32),
            pltpu.VMEM((share, channels), f32),
            dma((15,)),
            dma((6,)),
            dma((ny - 1, heads)),
            dma((1 + 3 * heads,)),
            dma((ny - 1, heads)),
            dma((nz - 1, cuts)),
            dma((1,)),
        ],
        compiler_params=pltpu.CompilerParams(
            collective_id=0, has_side_effects=True, vmem_limit_bytes=32 * 1024 * 1024
        ),
        name="block",
    )(*[pltpu.with_memory_space_constraint(operand, pltpu.HBM) for operand in operands])
    return (block_out[None], velocity)


def solution(mesh):
    in_specs = (
        P("cfg", "ctx", "tp"),
        P("cfg", "ctx", "tp"),
        P("cfg", "ctx", "tp"),
        P(),
        P(),
        P("cfg", ("ctx", "tp"), None),
        P("cfg", ("ctx", "tp"), None),
        P("cfg", "ctx"),
        P("cfg", None),
        P("tp", None),
        P("cfg", None),
        P("cfg", None),
        P(),
    )
    out_specs = (P("cfg", ("ctx", "tp"), None), P(("ctx", "tp"), "cfg"))
    return jax.shard_map(shards, mesh=mesh, in_specs=in_specs, out_specs=out_specs, check_vma=False)
```

```python
import functools
import math

import jax
import jax.numpy as jnp
from jax import lax
from jax.experimental import pallas as pl
from jax.experimental.pallas import tpu as pltpu
from jax.sharding import PartitionSpec as P

guidance_scale = 3.0
f32 = jnp.float32
bf16 = jnp.bfloat16
cut = 512


def dot(a, b, contract=(1, 0)):
    return lax.dot_general(
        a, b, (((contract[0],), (contract[1],)), ((), ())), preferred_element_type=f32
    )


def remote(src, dst, sems, kind, index, device):
    return pltpu.make_async_remote_copy(
        src_ref=src,
        dst_ref=dst,
        send_sem=sems[0].at[kind],
        recv_sem=sems[1].at[index],
        device_id=device,
        device_id_type=pl.DeviceIdType.MESH,
    )


def kernel(
    ny,
    nz,
    q_hbm,
    k_hbm,
    v_hbm,
    qg_hbm,
    kg_hbm,
    mask_hbm,
    gate_hbm,
    shift_hbm,
    scale_hbm,
    bi_hbm,
    co_hbm,
    w_hbm,
    pw_hbm,
    bo_out,
    vel_out,
    bo_ref,
    vel_ref,
    q_ref,
    k_ref,
    v_ref,
    qg_ref,
    kg_ref,
    mask_ref,
    gate_ref,
    shift_ref,
    scale_ref,
    bi_ref,
    co_ref,
    w_ref,
    pw_ref,
    sel_ref,
    kbuf,
    vbuf,
    rk,
    rv,
    qbuf,
    oacc,
    stat,
    part_o,
    part_s,
    own_o,
    own_s,
    osnd,
    orcv,
    att_ref,
    pbuf,
    zsnd,
    zrcv,
    ysnd,
    yrcv,
    loc_sem,
    left,
    qr,
    kr,
    or_,
    zr,
    yr,
):
    count, width = q_ref.shape
    depth = qg_ref.shape[1]
    heads = width // depth
    live = qbuf.shape[3]
    share, feats = bi_ref.shape
    cuts = feats // cut
    c2 = depth ** (-0.5) * math.log2(math.e)
    yh, zh = ny // 2, nz // 2

    cfg = lax.axis_index("cfg")
    ctx = lax.axis_index("ctx")
    tp = lax.axis_index("tp")
    core = lax.rem(ctx, 2)
    hi = lax.rem(lax.div(ctx, 2), 2)
    y = lax.div(ctx, 4)
    x = hi * 2 + cfg

    def at_x(place):
        return {"cfg": lax.rem(place, 2), "ctx": y * 4 + lax.div(place, 2) * 2 + 1 - core}

    x_up, x_dn = at_x(lax.rem(x + 1, 4)), at_x(lax.rem(x + 3, 4))
    sib = {"ctx": ctx + 1 - 2 * core}
    y_up = {"ctx": lax.rem(y + 1, ny) * 4 + hi * 2 + 1 - core}
    y_dn = {"ctx": lax.rem(y + ny - 1, ny) * 4 + hi * 2 + 1 - core}
    z_up = {"tp": lax.rem(tp + 1, nz)}
    z_dn = {"tp": lax.rem(tp + nz - 1, nz)}
    other = {"cfg": 1 - cfg}

    barrier = pltpu.get_barrier_semaphore()
    for device in (x_up, x_dn, sib, y_up, y_dn, z_up, z_dn, other):
        pl.semaphore_signal(
            barrier, inc=1, device_id=device, device_id_type=pl.DeviceIdType.MESH
        )

    pairs = (
        (mask_hbm, mask_ref),
        (q_hbm, q_ref),
        (qg_hbm, qg_ref),
        (k_hbm, k_ref),
        (kg_hbm, kg_ref),
        (v_hbm, v_ref),
        (w_hbm, w_ref),
        (bi_hbm, bi_ref),
        (co_hbm, co_ref),
        (gate_hbm, gate_ref),
        (scale_hbm, scale_ref),
        (shift_hbm, shift_ref),
        (pw_hbm, pw_ref),
    )
    loads = [
        pltpu.make_async_copy(src, dst, loc_sem.at[n]) for n, (src, dst) in enumerate(pairs)
    ]
    for load in loads:
        load.start()

    def q_up(s, h):
        return remote(
            qbuf.at[lax.rem(ny - s, ny), h], qbuf.at[ny - 1 - s, h], (left, qr), 0, (s, h), y_up
        )

    def q_dn(s, h):
        return remote(qbuf.at[s, h], qbuf.at[s + 1, h], (left, qr), 0, (yh + s, h), y_dn)

    kv = (left, kr)
    first_leg, second_leg, third_leg = 1, 1 + heads, 1 + 2 * heads

    def k_sib(h):
        return remote(kbuf.at[0, h], kbuf.at[1, h], kv, 1, 0, sib)

    def v_sib(h):
        return remote(vbuf.at[0, h], vbuf.at[1, h], kv, 2, 0, sib)

    def k_out(h):
        return remote(kbuf.at[0, h], rk.at[h], kv, 1, first_leg + h, x_up)

    def v_out(h):
        return remote(vbuf.at[0, h], rv.at[h], kv, 2, first_leg + h, x_dn)

    def k_on(h):
        return remote(rk.at[h], kbuf.at[2, h], kv, 1, second_leg + h, x_up)

    def v_on(h):
        return remote(rv.at[h], vbuf.at[2, h], kv, 2, second_leg + h, x_dn)

    def k_last(h):
        return remote(kbuf.at[2, h], kbuf.at[3, h], kv, 1, third_leg + h, sib)

    def v_last(h):
        return remote(vbuf.at[2, h], vbuf.at[3, h], kv, 2, third_leg + h, sib)

    def kv_come(n, index):
        block = kbuf.at[0, 0:2] if n == 1 else kbuf.at[0:2]
        remote(block, block, kv, 1, index, sib).wait_recv()

    def o_up(s, h):
        return remote(osnd.at[s, h], orcv.at[s, h], (left, or_), 3, (s, h), y_up)

    def o_dn(s, h):
        return remote(
            osnd.at[yh + s, h], orcv.at[yh + s, h], (left, or_), 3, (yh + s, h), y_dn
        )

    def z_upc(s, n):
        return remote(zsnd.at[s, n], zrcv.at[s, n], (left, zr), 4, (s, n), z_up)

    def z_dnc(s, n):
        place = nz - 2 - s
        return remote(zsnd.at[place, n], zrcv.at[place, n], (left, zr), 4, (place, n), z_dn)

    loads[0].wait()
    alive = (mask_ref[...] == 0).astype(f32)
    alive8 = jnp.broadcast_to(alive, (8, count))
    before = (
        lax.broadcasted_iota(jnp.int32, (count, count), 0)
        < lax.broadcasted_iota(jnp.int32, (count, count), 1)
    ).astype(f32)
    rank = dot(alive8.astype(bf16), before.astype(bf16))[0:1]
    slot = lax.broadcasted_iota(jnp.int32, (live, count), 0).astype(f32)
    picks = jnp.where((slot == rank) & (alive > 0.5), 1.0, 0.0)
    sel_ref[...] = picks.T.astype(bf16)
    picks = picks.astype(bf16)

    def normed_head(ref, gain_ref, h):
        part = ref[:, h * depth : (h + 1) * depth].astype(f32)
        square = jnp.mean(part * part, axis=-1, keepdims=True)
        return part * lax.rsqrt(square + 1e-06) * gain_ref[...]

    for load in loads[1:3]:
        load.wait()
    for h in range(heads):
        qn = normed_head(q_ref, qg_ref, h).astype(bf16)
        qbuf[0, h] = dot(picks, qn).T.astype(bf16)
    pl.semaphore_wait(barrier, 8)
    for h in range(heads):
        q_up(0, h).start()
        q_dn(0, h).start()
    for load in loads[3:6]:
        load.wait()
    for h in range(heads):
        kbuf[0, h] = normed_head(k_ref, kg_ref, h).astype(bf16)
        vbuf[0, h] = v_ref[:, h * depth : (h + 1) * depth].astype(f32).T.astype(bf16)
    for h in range(heads):
        k_out(h).start()
        v_out(h).start()
        k_sib(h).start()
        v_sib(h).start()

    def lanes(ref, places, *index):
        parts = [ref[(place, *index)] for place in places]
        return parts[0] if len(parts) == 1 else jnp.concatenate(parts, axis=1)

    def sums(places, slots, stored, which=range(heads)):
        def scores_of(h):
            queries = lanes(qbuf, places, h)
            return [dot(kbuf[j, h], queries) for j in slots]

        which = list(which)
        ahead = scores_of(which[0])
        for n, h in enumerate(which):
            scores = ahead
            if n + 1 < len(which):
                ahead = scores_of(which[n + 1])
            top = functools.reduce(
                jnp.maximum, [jnp.max(s, axis=0, keepdims=True) for s in scores]
            )
            top = top.astype(bf16).astype(f32)
            if stored:
                old = lanes(stat, places, h, slice(0, 1))
                top = jnp.maximum(top, old)
            weights = [jnp.exp2((s - top) * c2) for s in scores]
            total = sum(jnp.sum(w, axis=0, keepdims=True) for w in weights)
            summed = sum(dot(vbuf[j, h], w.astype(bf16)) for j, w in zip(slots, weights))
            if stored:
                factor = jnp.exp2((old - top) * c2)
                total += factor * lanes(stat, places, h, slice(1, 2))
                summed += factor * lanes(oacc, places, h)
            yield summed, top, total

    def near(*places):
        for h, (summed, top, total) in enumerate(sums(places, (0, 1), False)):
            for n, place in enumerate(places):
                part = slice(n * live, (n + 1) * live)
                oacc[place, h] = summed[:, part]
                stat[place, h, 0:1] = top[:, part]
                stat[place, h, 1:2] = total[:, part]

    def relay(g):
        kv_come(1, first_leg + g)
        k_on(g).start()
        v_on(g).start()

    def last_leg(g):
        kv_come(1, second_leg + g)
        k_last(g).start()
        v_last(g).start()

    def q_pass(s):
        for h in range(heads):
            q_up(s, h).wait_recv()
            q_up(s + 1, h).start()
            q_dn(s, h).wait_recv()

            @pl.when(s < yh - 2)
            def _():
                q_dn(s + 1, h).start()

            if h < heads - 1:

                @pl.when(s == yh - 2)
                def _():
                    last_leg(h)

    kv_come(heads, 0)
    near(0)

    def q_step(s, carry):
        @pl.when(s == 1)
        def _():
            relay(1)

        q_pass(s)

        @pl.when(s == 0)
        def _():
            relay(0)

        @pl.when(s == 1)
        def _():
            relay(2)

        near(ny - 1 - s, s + 1)
        return carry

    lax.fori_loop(0, yh - 1, q_step, 0)
    last_leg(2)

    def put(way, s, h, summed, top, total):
        osnd[way * yh + s, h, 0:depth] = summed.astype(bf16)
        high = total.astype(bf16).astype(f32)
        row = lax.broadcasted_iota(jnp.int32, (16, live), 0)
        tile = jnp.where(row == 0, top, jnp.where(row == 1, high, total - high))
        osnd[way * yh + s, h, depth : depth + 16] = tile.astype(bf16)

    def merge(way, s, h, summed, top, total):
        theirs = orcv[way * yh + s, h, 0:depth].astype(f32)
        tile = orcv[way * yh + s, h, depth : depth + 16].astype(f32)
        their_top, their_total = tile[0:1], tile[1:2] + tile[2:3]
        newest = jnp.maximum(top, their_top)
        mine, factor = jnp.exp2((top - newest) * c2), jnp.exp2((their_top - newest) * c2)
        return summed * mine + theirs * factor, newest, total * mine + their_total * factor

    for h in range(heads):
        q_up(yh - 1, h).wait_recv()
        kv_come(1, third_leg + h)
        for parts in sums((yh,), range(4), False, (h,)):
            put(0, 0, h, *parts)
            o_up(0, h).start()
    for h, parts in enumerate(sums((yh + 1,), (2, 3), True)):
        put(1, 0, h, *parts)
        o_dn(0, h).start()

    def own_sums(s):
        places = (yh - s, lax.rem(yh + 1 + s, ny))
        for h, (summed, top, total) in enumerate(sums(places, (2, 3), True)):
            part_o[lax.rem(s, 2), h] = summed
            part_s[lax.rem(s, 2), h, 0:1] = top
            part_s[lax.rem(s, 2), h, 1:2] = total

    def own_part(s, h, way):
        side = slice(way * live, (way + 1) * live)
        step = lax.rem(s, 2)
        return part_o[step, h, :, side], part_s[step, h, 0:1, side], part_s[step, h, 1:2, side]

    own_sums(1)

    def o_step(s, carry):
        for h in range(heads):
            o_up(s - 1, h).wait_recv()
            put(0, s, h, *merge(0, s - 1, h, *own_part(s, h, 0)))
            o_up(s, h).start()

        @pl.when(s < yh - 1)
        def _():
            own_sums(s + 1)

        for h in range(heads):
            o_dn(s - 1, h).wait_recv()
            below = merge(1, s - 1, h, *own_part(s, h, 1))

            @pl.when(s < yh - 1)
            def _():
                put(1, s, h, *below)
                o_dn(s, h).start()

            own_o[h], own_s[h, 0:1], own_s[h, 1:2] = below
        return carry

    lax.fori_loop(1, yh, o_step, 0)

    for h in range(heads):
        o_up(yh - 1, h).wait_recv()
        summed, top, total = merge(0, yh - 1, h, own_o[h], own_s[h, 0:1], own_s[h, 1:2])
        done = (summed / total).astype(bf16)
        att_ref[:, h * depth : (h + 1) * depth] = dot(sel_ref[...], done, (1, 1)).astype(bf16)

    loads[6].wait()

    def rows_of(n, place):
        start = pl.multiple_of(place * share, share)
        return pbuf[n, pl.ds(start, share), :]

    def hops(n):
        odd = lax.rem(n, 2)
        return zh - odd, zh - 1 + odd

    def z_first(n, carry):
        up, down = hops(n)
        columns = pl.ds(pl.multiple_of(n * cut, cut), cut)
        pbuf[n] = dot(att_ref[...], w_ref[:, columns])
        zsnd[0, n] = rows_of(n, lax.rem(tp + up, nz)).astype(bf16)
        z_upc(0, n).start()
        zsnd[nz - 2, n] = rows_of(n, lax.rem(tp + nz - down, nz)).astype(bf16)
        z_dnc(0, n).start()
        return carry

    lax.fori_loop(0, cuts, z_first, 0)

    def passed(place, n, dest):
        return rows_of(n, dest) + zrcv[place, n].astype(f32)

    def z_step(s, carry):
        def z_cut(n, inner):
            up, down = hops(n)
            z_upc(s - 1, n).wait_recv()
            z_dnc(s - 1, n).wait_recv()
            above = passed(s - 1, n, lax.rem(tp + up - s, nz))
            below = passed(nz - 1 - s, n, lax.rem(tp + nz - down + s, nz))
            zsnd[s, n] = above.astype(bf16)
            zsnd[nz - 2 - s, n] = below.astype(bf16)
            z_upc(s, n).start()
            z_dnc(s, n).start()
            return inner

        return lax.fori_loop(0, cuts, z_cut, carry)

    lax.fori_loop(1, zh - 1, z_step, 0)

    for n in range(cuts):
        if n % 2 == 0:
            z_upc(zh - 2, n).wait_recv()
            zsnd[zh - 1, n] = passed(zh - 2, n, lax.rem(tp + 1, nz)).astype(bf16)
            z_upc(zh - 1, n).start()
        else:
            z_dnc(zh - 2, n).wait_recv()
            zsnd[zh - 1, n] = passed(zh, n, lax.rem(tp + nz - 1, nz)).astype(bf16)
            z_dnc(zh - 1, n).start()

    for load in loads[7:]:
        load.wait()
    own_rows = pl.ds(pl.multiple_of(tp * share, share), share)
    alive_rows = jnp.sum(sel_ref[own_rows, :].astype(f32), axis=1, keepdims=True) > 0.5
    sums = jnp.zeros((share, 1), f32)
    for n in range(cuts):
        columns = slice(n * cut, (n + 1) * cut)
        up, down = zh - n % 2, zh - 1 + n % 2
        z_upc(up - 1, n).wait_recv()
        z_dnc(down - 1, n).wait_recv()
        projected = (
            rows_of(n, tp) + zrcv[up - 1, n].astype(f32) + zrcv[nz - 1 - down, n].astype(f32)
        )
        mixed = bi_ref[:, columns].astype(f32) + gate_ref[:, columns] * projected
        out = jnp.where(alive_rows, mixed, co_ref[:, columns].astype(f32)).astype(bf16)
        bo_ref[:, columns] = out
        sums += jnp.sum(out.astype(f32), axis=1, keepdims=True)
    store = pltpu.make_async_copy(bo_ref, bo_out, loc_sem.at[13])
    store.start()
    center = sums * (1.0 / feats)
    away = bo_ref[...].astype(f32) - center
    spread = jnp.mean(away * away, axis=1, keepdims=True)
    normed = away * lax.rsqrt(spread + 1e-06) * (1.0 + scale_ref[...]) + shift_ref[...]
    ysnd[...] = dot(normed.astype(bf16), pw_ref[...], (1, 1))
    swap = remote(ysnd, yrcv, (left, yr), 5, 0, other)
    swap.start()

    for kind, sent in enumerate(
        (qbuf.at[0 : ny - 1], kbuf, vbuf, osnd, zsnd)
    ):
        remote(sent, sent, (left, qr), kind, (0, 0), sib).wait_send()
    swap.wait()
    mine, theirs = ysnd[...], yrcv[...]
    cond = jnp.where(cfg == 0, mine, theirs)
    uncond = jnp.where(cfg == 0, theirs, mine)
    velocity = uncond + guidance_scale * (cond - uncond)
    half_width = vel_ref.shape[1]
    vel_ref[...] = jnp.where(cfg == 0, velocity[:, :half_width], velocity[:, half_width:])
    last = pltpu.make_async_copy(vel_ref, vel_out, loc_sem.at[14])
    last.start()
    store.wait()
    last.wait()


def hand_over(a_ref, b_ref, a_out, b_out, sems):
    copies = (
        pltpu.make_async_copy(a_ref, a_out, sems.at[0]),
        pltpu.make_async_copy(b_ref, b_out, sems.at[1]),
    )
    for copy in copies:
        copy.start()
    for copy in copies:
        copy.wait()


def shards(
    query_proj,
    key_proj,
    value_proj,
    query_gain,
    key_gain,
    block_input,
    cached_out,
    replay_mask,
    branch_gate,
    attn_weight,
    final_shift,
    final_scale,
    patch_weight,
):
    ny = lax.axis_size("ctx") // 4
    nz = lax.axis_size("tp")
    count, width = query_proj.shape[1:]
    depth = query_gain.shape[0]
    heads = width // depth
    live = count // 2
    share, feats = block_input.shape[1:]
    channels = patch_weight.shape[1]
    yh, zh = ny // 2, nz // 2
    cuts = feats // cut
    anywhere = pl.BlockSpec(memory_space=pl.ANY)
    hbm = pl.BlockSpec(memory_space=pltpu.HBM)
    dma = pltpu.SemaphoreType.DMA
    operands = (
        query_proj[0],
        key_proj[0],
        value_proj[0],
        query_gain[None],
        key_gain[None],
        replay_mask,
        branch_gate,
        final_shift,
        final_scale,
        block_input[0],
        cached_out[0],
        attn_weight,
        patch_weight.T,
    )
    block_out, velocity = pl.pallas_call(
        functools.partial(kernel, ny, nz),
        out_shape=(
            jax.ShapeDtypeStruct((share, feats), bf16),
            jax.ShapeDtypeStruct((share, channels // 2), f32),
        ),
        in_specs=[hbm] * 13,
        out_specs=(anywhere, anywhere),
        scratch_shapes=[
            pltpu.VMEM((share, feats), bf16),
            pltpu.VMEM((share, channels // 2), f32),
            *[pltpu.VMEM((count, width), bf16)] * 3,
            *[pltpu.VMEM((1, depth), f32)] * 2,
            pltpu.VMEM((1, count), jnp.int32),
            *[pltpu.VMEM((1, feats), f32)] * 3,
            *[pltpu.VMEM((share, feats), bf16)] * 2,
            pltpu.VMEM((width, feats), bf16),
            pltpu.VMEM((channels, feats), bf16),
            pltpu.VMEM((count, live), bf16),
            pltpu.VMEM((4, heads, count, depth), bf16),
            pltpu.VMEM((4, heads, depth, count), bf16),
            pltpu.VMEM((heads, count, depth), bf16),
            pltpu.VMEM((heads, depth, count), bf16),
            pltpu.VMEM((ny, heads, depth, live), bf16),
            pltpu.VMEM((ny, heads, depth, live), f32),
            pltpu.VMEM((ny, heads, 8, live), f32),
            pltpu.VMEM((2, heads, depth, 2 * live), f32),
            pltpu.VMEM((2, heads, 8, 2 * live), f32),
            pltpu.VMEM((heads, depth, live), f32),
            pltpu.VMEM((heads, 8, live), f32),
            *[pltpu.VMEM((ny - 1, heads, depth + 16, live), bf16)] * 2,
            pltpu.VMEM((count, width), bf16),
            pltpu.VMEM((cuts, count, cut), f32),
            *[pltpu.VMEM((nz - 1, cuts, share, cut), bf16)] * 2,
            pltpu.VMEM((share, channels), f32),
            pltpu.VMEM((share, channels), f32),
            dma((15,)),
            dma((6,)),
            dma((ny - 1, heads)),
            dma((1 + 3 * heads,)),
            dma((ny - 1, heads)),
            dma((nz - 1, cuts)),
            dma((1,)),
        ],
        compiler_params=pltpu.CompilerParams(
            collective_id=0, has_side_effects=True, vmem_limit_bytes=32 * 1024 * 1024
        ),
        name="block",
    )(*[pltpu.with_memory_space_constraint(operand, pltpu.HBM) for operand in operands])
    vmem = pl.BlockSpec(memory_space=pl.ANY)
    block_out, velocity = pl.pallas_call(
        hand_over,
        out_shape=(
            jax.ShapeDtypeStruct(block_out.shape, bf16),
            jax.ShapeDtypeStruct(velocity.shape, f32),
        ),
        in_specs=[vmem] * 2,
        out_specs=(hbm, hbm),
        scratch_shapes=[dma((2,))],
        name="hand_over",
    )(*[pltpu.with_memory_space_constraint(part, pltpu.VMEM) for part in (block_out, velocity)])
    return (block_out[None], velocity)


def solution(mesh):
    in_specs = (
        P("cfg", "ctx", "tp"),
        P("cfg", "ctx", "tp"),
        P("cfg", "ctx", "tp"),
        P(),
        P(),
        P("cfg", ("ctx", "tp"), None),
        P("cfg", ("ctx", "tp"), None),
        P("cfg", "ctx"),
        P("cfg", None),
        P("tp", None),
        P("cfg", None),
        P("cfg", None),
        P(),
    )
    out_specs = (P("cfg", ("ctx", "tp"), None), P(("ctx", "tp"), "cfg"))
    return jax.shard_map(shards, mesh=mesh, in_specs=in_specs, out_specs=out_specs, check_vma=False)
```
